128 devices in a mesh: dp: 8 (over z_hi, y), tensor: 16 (over x, z_lo, core).
Axes of the slice: x: 4, y: 4, z: 4 (z_hi: 2, z_lo: 2; z = z_hi * 2 + z_lo), core: 2. Of those that a mesh axis runs over, the one named last changes fastest.
Arguments:
- noisy: bfloat16 [64, 256, 1152], P('dp', None, 'tensor'), may hold values from -6 to 6
- labels: int32 [64], P('dp'), may hold values from 0 to 999
- tsteps: int32 [64], P('dp'), may hold values from 0 to 999
- guide_index: int32 [64], P('dp'), may hold values from 0 to 31
- class_table: bfloat16 [1001, 1152], replicated, may hold values from -6 to 6
- time_table: bfloat16 [1000, 1152], replicated, may hold values from -6 to 6
- guide_table: bfloat16 [32, 1152], replicated, may hold values from -6 to 6
- guide_weights: float32 [32], replicated, may hold values from 0.5 to 4
- teacher_qkv: bfloat16 [1152, 3456], P(None, 'tensor'), may hold values from -0.1875 to 0.1875
- teacher_out: bfloat16 [1152, 1152], P('tensor'), may hold values from -0.1875 to 0.1875
- teacher_ada: bfloat16 [3, 1152, 1152], P(None, None, 'tensor'), may hold values from -0.1875 to 0.1875
- student_qkv: bfloat16 [1152, 3456], P(None, 'tensor'), may hold values from -0.1875 to 0.1875
- student_out: bfloat16 [1152, 1152], P('tensor'), may hold values from -0.1875 to 0.1875
- student_ada: bfloat16 [3, 1152, 1152], P(None, None, 'tensor'), may hold values from -0.1875 to 0.1875
Outputs:
- grad_qkv: float32 [1152, 3456], P('dp', 'tensor')
- grad_out: float32 [1152, 1152], P('tensor', 'dp')
- grad_ada: float32 [3, 1152, 1152], P(None, 'dp', 'tensor')
The draws below stay inside these ranges and needn't reach their ends.
All inputs are finite; a program needn't handle non-finite values.
Results may differ from the reference program's by a relative error of at most 0.034.
Values may be sent and summed in bfloat16 or wider, within the bound.
No kernel may reach another device: no remote copies, remote signals or barrier semaphores. Data moves between devices by JAX's collectives and lax.ppermute only.
A program may use at most 128 MiB of HBM per device.

```python
import math
import jax
import jax.numpy as jnp
from jax import lax

D = 1152
HEADS = 16
HD = 72
CLASSES = 1000
L = 256
TSTEPS = 1000
GUIDES = 32
BATCH = 64
N_TENSOR = 16


def touch_ends(values, key, smallest, high):
    longest = values.shape.index(max(values.shape))
    spots = []
    for shift in (0, 1):
        where = [jax.random.randint(jax.random.fold_in(key, axis), (), 0, length) for axis, length in enumerate(values.shape)]
        where[longest] = (where[longest] + shift) % values.shape[longest]
        spots.append(tuple(where))
    return values.at[spots[0]].set(smallest).at[spots[1]].set(high)


def block_scale(stream_key, shape, pieces, low, largest):
    gain = 1.0
    for position, parts in pieces:
        steps = jax.random.uniform(jax.random.fold_in(jax.random.fold_in(stream_key, 6), position), (parts,), jnp.float32, low / len(pieces), largest / len(pieces))
        gain = gain * jnp.repeat(jnp.exp(steps), shape[position] // parts).reshape((-1,) + (1,) * (len(shape) - 1 - position))
    return gain


def normal_values(rng, dims, scale, limit, cuts=(), dtype=jnp.bfloat16):
    result = scale * jax.random.normal(rng, dims, jnp.float32)
    if cuts:
        result = result * block_scale(rng, dims, cuts, -0.22, 0.18)
    return jnp.clip(result, -limit, limit).astype(dtype)


def setup_inputs(seed: int = 0) -> dict:
    key_list = jax.random.split(jax.random.key(seed), 15)
    noisy = normal_values(key_list[0], (BATCH, L, D), 1.0, 6.0, ((0, 8), (2, 16)))
    labels = touch_ends(jax.random.randint(key_list[1], (BATCH,), 0, CLASSES), jax.random.fold_in(key_list[1], 1), 0, CLASSES - 1).astype(jnp.int32)
    tsteps = touch_ends(jax.random.randint(key_list[2], (BATCH,), 0, TSTEPS), jax.random.fold_in(key_list[2], 1), 0, TSTEPS - 1).astype(jnp.int32)
    guide_index = touch_ends(jax.random.randint(key_list[3], (BATCH,), 0, GUIDES), jax.random.fold_in(key_list[3], 1), 0, GUIDES - 1).astype(jnp.int32)
    class_table = normal_values(key_list[4], (CLASSES + 1, D), 1.0, 6.0)
    time_table = normal_values(key_list[5], (TSTEPS, D), 1.0, 6.0)
    guide_table = normal_values(key_list[6], (GUIDES, D), 1.0, 6.0)
    guide_weights = jnp.clip(jax.random.uniform(key_list[7], (GUIDES,), jnp.float32, 0.5, 4.0), 0.5, 4.0)
    teacher_qkv = normal_values(key_list[8], (D, 3 * D), D ** -0.5, 0.1875, ((1, 16),))
    teacher_out = normal_values(key_list[9], (D, D), D ** -0.5, 0.1875, ((0, 16),))
    teacher_ada = normal_values(key_list[10], (3, D, D), D ** -0.5, 0.1875, ((2, 16),))
    student_qkv = normal_values(key_list[11], (D, 3 * D), D ** -0.5, 0.1875, ((1, 16),))
    student_out = normal_values(key_list[12], (D, D), D ** -0.5, 0.1875, ((0, 16),))
    student_ada = normal_values(key_list[13], (3, D, D), D ** -0.5, 0.1875, ((2, 16),))
    return dict(noisy=noisy, labels=labels, tsteps=tsteps, guide_index=guide_index, class_table=class_table, time_table=time_table, guide_table=guide_table, guide_weights=guide_weights, teacher_qkv=teacher_qkv, teacher_out=teacher_out, teacher_ada=teacher_ada, student_qkv=student_qkv, student_out=student_out, student_ada=student_ada)


norm_eps = 1e-06

def round_trip(value):
    return lax.optimization_barrier(value.astype(jnp.bfloat16)).astype(jnp.float32)

def block_sum(left_rows, right_rows, block_count):
    inner_width = left_rows.shape[1] // block_count

    def add_block(block_idx, running):
        offset = (block_idx * inner_width).astype(jnp.int32)
        left_block = lax.dynamic_slice_in_dim(left_rows, offset, inner_width, 1)
        right_block = lax.dynamic_slice_in_dim(right_rows, offset, inner_width, 0)
        partial_value = jnp.dot(left_block, right_block, preferred_element_type=jnp.float32)
        return running + round_trip(partial_value)
    initial = jnp.zeros((left_rows.shape[0], right_rows.shape[1]), jnp.float32)
    return lax.fori_loop(0, block_count, add_block, initial)

def sample_probs(sample_qkv):
    queries = sample_qkv[:, :, 0].astype(jnp.float32)
    key_rows = sample_qkv[:, :, 1].astype(jnp.float32)
    scores = jnp.einsum('lhe,mhe->hlm', queries, key_rows) * (1.0 / math.sqrt(HD))
    exponent = jnp.exp(scores - lax.optimization_barrier(jnp.max(scores, axis=-1, keepdims=True)))
    return exponent / lax.optimization_barrier(jnp.sum(exponent, axis=-1, keepdims=True))

def attend_one(sample_qkv):
    attn_prob = sample_probs(sample_qkv)
    values = sample_qkv[:, :, 2].astype(jnp.float32)
    attn_mixed = jnp.einsum('hlm,mhe->lhe', round_trip(attn_prob), values)
    return attn_mixed.astype(jnp.bfloat16)

def attend_back(sample_pair):
    sample_qkv, grad_low = sample_pair
    attn_prob = sample_probs(sample_qkv)
    prob_low = round_trip(attn_prob)
    queries = sample_qkv[:, :, 0].astype(jnp.float32)
    key_rows = sample_qkv[:, :, 1].astype(jnp.float32)
    values = sample_qkv[:, :, 2].astype(jnp.float32)
    grad_mixed = grad_low.astype(jnp.float32)
    grad_probs = jnp.einsum('lhe,mhe->hlm', grad_mixed, values)
    row_delta = lax.optimization_barrier(jnp.sum(attn_prob * grad_probs, axis=-1, keepdims=True))
    grad_scores = round_trip(attn_prob * (grad_probs - row_delta) * (1.0 / math.sqrt(HD)))
    grad_query = jnp.einsum('hlm,mhe->lhe', grad_scores, key_rows)
    grad_keys = jnp.einsum('hlm,lhe->mhe', grad_scores, queries)
    grad_values = jnp.einsum('hlm,lhe->mhe', prob_low, grad_mixed)
    return jnp.stack([grad_query, grad_keys, grad_values], axis=2).astype(jnp.bfloat16)

def forward(normed, embed_act, qkv_weight, out_weight, ada_weight):
    batch_size = normed.shape[0]
    modulation = jnp.einsum('bd,kde->bke', embed_act.astype(jnp.float32), ada_weight.astype(jnp.float32))
    modulated = (normed.astype(jnp.float32) * (1.0 + modulation[:, 1][:, None]) + modulation[:, 0][:, None]).astype(jnp.bfloat16)
    qkv_sums = jnp.dot(modulated.reshape(-1, D), qkv_weight, preferred_element_type=jnp.float32)
    heads_qkv = qkv_sums.astype(jnp.bfloat16).reshape(batch_size, L, HEADS, 3, HD)
    attn_mixed = lax.map(attend_one, heads_qkv).reshape(-1, D)
    projected = block_sum(attn_mixed, out_weight, N_TENSOR).reshape(batch_size, L, D)
    branch = modulation[:, 2][:, None] * projected
    return (branch, modulated, heads_qkv, attn_mixed, projected, modulation)

def reference(noisy, labels, tsteps, guide_index, class_table, time_table, guide_table, guide_weights, teacher_qkv, teacher_out, teacher_ada, student_qkv, student_out, student_ada):
    batch_size = noisy.shape[0]
    signal = noisy.astype(jnp.float32)
    row_mean = lax.optimization_barrier(jnp.sum(signal, axis=2, keepdims=True)) / D
    row_var = lax.optimization_barrier(jnp.sum(signal * signal, axis=2, keepdims=True)) / D - row_mean * row_mean
    normed = ((signal - row_mean) * lax.rsqrt(row_var + norm_eps)).astype(jnp.bfloat16)
    time_embed = time_table[tsteps].astype(jnp.float32)
    cond_embed = class_table[labels].astype(jnp.float32) + time_embed
    null_embed = class_table[CLASSES].astype(jnp.float32)[None, :] + time_embed
    student_embed = cond_embed + guide_table[guide_index].astype(jnp.float32)
    cond_act = jax.nn.silu(cond_embed).astype(jnp.bfloat16)
    null_act = jax.nn.silu(null_embed).astype(jnp.bfloat16)
    student_act = jax.nn.silu(student_embed).astype(jnp.bfloat16)
    cond_result = forward(normed, cond_act, teacher_qkv, teacher_out, teacher_ada)
    null_result = forward(normed, null_act, teacher_qkv, teacher_out, teacher_ada)
    cond_update = round_trip(cond_result[0])
    null_update = round_trip(null_result[0])
    strength = guide_weights[guide_index][:, None, None]
    target = signal + ((1.0 + strength) * cond_update - strength * null_update)
    branch, modulated, heads_qkv, attn_mixed, projected, modulation = forward(normed, student_act, student_qkv, student_out, student_ada)
    cotangent = (signal + branch - target) * (1.0 / math.sqrt(batch_size * L))
    grad_gate = lax.optimization_barrier(jnp.sum(cotangent * projected, axis=1))
    grad_proj = (cotangent * modulation[:, 2][:, None]).astype(jnp.bfloat16).reshape(-1, D)
    grad_out = jnp.dot(attn_mixed.T, grad_proj, preferred_element_type=jnp.float32)
    grad_mixed = jnp.dot(grad_proj, student_out.T, preferred_element_type=jnp.float32)
    grad_low = grad_mixed.astype(jnp.bfloat16).reshape(batch_size, L, HEADS, HD)
    grad_qkv_act = lax.map(attend_back, (heads_qkv, grad_low)).reshape(-1, 3 * D)
    grad_qkv = jnp.dot(modulated.reshape(-1, D).T, grad_qkv_act, preferred_element_type=jnp.float32)
    grad_input = block_sum(grad_qkv_act, student_qkv.T, N_TENSOR).reshape(batch_size, L, D)
    grad_shift = lax.optimization_barrier(jnp.sum(grad_input, axis=1))
    grad_scale = lax.optimization_barrier(jnp.sum(grad_input * normed.astype(jnp.float32), axis=1))
    grad_modulation = jnp.stack([grad_shift, grad_scale, grad_gate], axis=1)
    grad_ada = jnp.einsum('bd,bke->kde', student_act.astype(jnp.float32), grad_modulation, precision=lax.Precision.HIGHEST)
    return (grad_qkv, grad_out, grad_ada)
```

```python
import functools
import math

import jax
import jax.numpy as jnp
from jax import lax
from jax.experimental import pallas as pl
from jax.experimental.pallas import tpu as pltpu
from jax.sharding import Mesh
from jax.sharding import PartitionSpec as P

HD = 72
EPS = 1e-06
HEADS_HERE = 4
QKV = 3 * HD
F32 = jnp.float32
BF16 = jnp.bfloat16
SIZES = (2, 4, 4, 2, 2)
AXES = ("zhi", "y", "x", "zlo", "core")
DP = ("zhi", "y")
TENSOR = ("x", "zlo", "core")
QUAD = ("zlo", "core")
LANES = 384
KEPT = 40
INV_SQRT = 1.0 / math.sqrt(HD)


VM = pl.BlockSpec(memory_space=pltpu.VMEM)
SM = pl.BlockSpec(memory_space=pltpu.SMEM)


def params(mib, **kw):
    return pltpu.CompilerParams(vmem_limit_bytes=mib * 1024 * 1024, **kw)


def cost(us):
    return pl.CostEstimate(flops=int(us * 1e8), bytes_accessed=1000000, transcendentals=0)


def dot(a, b, ca, cb):
    return lax.dot_general(a, b, (((ca,), (cb,)), ((), ())), preferred_element_type=F32)


def shifted(n, k):
    return [(i, (i + k) % n) for i in range(n)]


def xored(n, k):
    return [(i, i ^ k) for i in range(n)]


def place(pos, pieces, whole):
    for shift, piece in zip((0, 3, 1, 2), pieces):
        rows = piece.shape[0]
        at = lax.rem(pos + shift, 4) * rows
        whole[pl.ds(pl.multiple_of(at, 32), rows), :] = piece[...]


def assemble_kernel(*refs):
    sources, (wq, wo), sems = refs[:8], refs[8:10], refs[10]
    copies = []
    for r in range(4):
        copies.append((sources[2 * r], wq.at[pl.ds(r * QKV, QKV), :]))
        copies.append((sources[2 * r + 1], wo.at[pl.ds(r * HD, HD), :]))
    copies = [pltpu.make_async_copy(a, b, sems.at[i]) for i, (a, b) in enumerate(copies)]
    for c in copies:
        c.start()
    for c in copies:
        c.wait()


def heads_forward(qkv_ref, mixed_ref, prob_ref):
    for h in range(HEADS_HERE):
        base = h * QKV
        q = qkv_ref[base : base + HD, :]
        k = qkv_ref[base + HD : base + 2 * HD, :]
        v = qkv_ref[base + 2 * HD : base + 3 * HD, :]
        s = dot(k, q, 0, 0) * INV_SQRT
        e = jnp.exp(s - jnp.max(s, axis=0, keepdims=True))
        prob = (e * (1.0 / jnp.sum(e, axis=0, keepdims=True))).astype(BF16)
        if prob_ref is not None:
            prob_ref[h] = prob
        mixed_ref[h * HD : (h + 1) * HD, :] = dot(v, prob, 1, 0).astype(BF16)


def student_kernel(
    image, col, scale_norm, pos_ref, p0, p1, p2, p3, mod_ref, wq_ref, wo_ref,
    normed_ref, modulated_ref, qkv_ref, prob_ref, mixed_ref, proj_ref, c_ref, x_ref,
):
    place(pos_ref[0], [p.at[image] for p in (p0, p1, p2, p3)], x_ref)
    width = x_ref.shape[0]
    x = x_ref[...].astype(F32)
    mean = jnp.sum(x, axis=0, keepdims=True) / width
    var = jnp.sum(x * x, axis=0, keepdims=True) / width - mean * mean
    normed = ((x - mean) * lax.rsqrt(var + EPS)).astype(BF16)
    normed_ref[...] = normed
    shift = mod_ref[:, col : col + 1]
    scale = mod_ref[:, col + 1 : col + 2]
    modulated_ref[...] = (normed.astype(F32) * (1.0 + scale) + shift).astype(BF16)
    qkv_ref[...] = dot(wq_ref[...], modulated_ref[...], 1, 0).astype(BF16)
    heads_forward(qkv_ref, mixed_ref, prob_ref)
    proj = dot(wo_ref[...], mixed_ref[...], 0, 0)
    proj_ref[...] = proj.astype(BF16)
    c_ref[...] = proj * (mod_ref[:, col + 2 : col + 3] * scale_norm)


def teacher_kernel(
    cols, pos_ref, coef_ref, normed_ref, mod_ref, wq_ref, wo_ref, cs_ref,
    o0, o1, o2, o3, acc_ref, modulated_ref, qkv_ref, mixed_ref,
):
    kind = pl.program_id(0)

    @pl.when(kind == 0)
    def _():
        acc_ref[...] = cs_ref[...]

    def column(m):
        return jnp.where(
            kind == 0, mod_ref[:, cols[0] + m : cols[0] + m + 1], mod_ref[:, cols[1] + m : cols[1] + m + 1]
        )

    modulated_ref[...] = (normed_ref[...].astype(F32) * (1.0 + column(1)) + column(0)).astype(BF16)
    qkv_ref[...] = dot(wq_ref[...], modulated_ref[...], 1, 0).astype(BF16)
    heads_forward(qkv_ref, mixed_ref, None)
    acc_ref[...] += dot(wo_ref[...], mixed_ref[...], 0, 0) * (column(2) * coef_ref[kind])

    @pl.when(kind == 1)
    def _():
        rows = o0.shape[0]
        for shift, out in zip((0, 1, 3, 2), (o0, o1, o2, o3)):
            at = lax.rem(pos_ref[0] + shift, 4) * rows
            out[...] = acc_ref[pl.ds(pl.multiple_of(at, 32), rows), :].astype(BF16)


def backward_kernel(
    col, pos_ref, p0, p1, p2, p3, mod_ref, wq_ref, wo_ref, normed_ref, qkv_ref, prob_ref, mixed_ref, proj_ref,
    gp_ref, gqkv_ref, rows_ref, cot_ref, glow_ref, gm_ref,
):
    place(pos_ref[0], (p0, p1, p2, p3), cot_ref)
    cot = cot_ref[...].astype(F32)
    gm_ref[:, 2:3] = jnp.sum(cot * proj_ref[...].astype(F32), axis=1, keepdims=True)
    gp_ref[...] = (cot * mod_ref[:, col + 2 : col + 3]).astype(BF16)
    glow_ref[...] = dot(wo_ref[...], gp_ref[...], 1, 0).astype(BF16)
    for h in range(HEADS_HERE):
        base = h * QKV
        q = qkv_ref[base : base + HD, :]
        k = qkv_ref[base + HD : base + 2 * HD, :]
        v = qkv_ref[base + 2 * HD : base + 3 * HD, :]
        g = glow_ref[h * HD : (h + 1) * HD, :]
        low = prob_ref[h]
        prob = low.astype(F32)
        gprob = dot(v, g, 0, 0)
        delta = jnp.sum(prob * gprob, axis=0, keepdims=True)
        gs = (prob * (gprob - delta) * INV_SQRT).astype(BF16)
        gqkv_ref[base : base + HD, :] = dot(k, gs, 1, 0).astype(BF16)
        gqkv_ref[base + HD : base + 2 * HD, :] = dot(q, gs, 1, 1).astype(BF16)
        gqkv_ref[base + 2 * HD : base + 3 * HD, :] = dot(g, low, 1, 1).astype(BF16)
    gin = dot(wq_ref[...], gqkv_ref[...], 0, 0)
    gm_ref[:, 0:1] = jnp.sum(gin, axis=1, keepdims=True)
    gm_ref[:, 1:2] = jnp.sum(gin * normed_ref[...].astype(F32), axis=1, keepdims=True)
    gm_ref[:, 3:] = jnp.zeros((gm_ref.shape[0], 125), F32)
    rows_ref[...] = gm_ref[...].T[:8]


def weight_grad(slot, operands, hq, ho):
    (m0, g0, p0, x0), (m1, g1, p1, x1) = operands
    a, b = slot * QKV, (slot + 1) * QKV
    hq[:, 0:QKV] = (dot(m0[...], g0[a:b, :], 1, 1) + dot(m1[...], g1[a:b, :], 1, 1)).astype(hq.dtype)
    a, b = slot * HD, (slot + 1) * HD
    ho[:, 0:HD] = (dot(p0[...], x0[a:b, :], 1, 1) + dot(p1[...], x1[a:b, :], 1, 1)).astype(ho.dtype)


def grads_kernel(m0, g0, p0, x0, m1, g1, p1, x1, s1, s3, s0, s2):
    for slot, out in ((1, s1), (3, s3), (0, s0), (2, s2)):
        weight_grad(slot, ((m0, g0, p0, x0), (m1, g1, p1, x1)), out.at[:, 0:256], out.at[:, 256:384])


def fold_kernel(at_ref, s0, s2, r1, r3, act_ref, a0, a1, a2, a3, out_ref):
    rows = (out_ref.shape[1] - 16) * 6 // 7
    width = a0.shape[1]
    summed = a0[...] + a1[...] + a2[...] + a3[...]
    side = lax.broadcasted_iota(jnp.int32, (16, 128), 1)
    part = rows // 6
    lane = lax.broadcasted_iota(jnp.int32, (rows, 128), 1)
    few = lane[:part]
    for dz, own, received in ((0, s0, r1), (1, s2, r3)):
        zlo = at_ref[1] if dz == 0 else 1 - at_ref[1]
        start = (at_ref[0] * 4 + zlo * 2 + at_ref[2]) * HD
        mine = pltpu.roll(summed, lax.rem(width - start, width), 1)[:, 0:128]
        mine = pltpu.roll(mine, 16, 1)

        def block(i, carry, own=own, received=received, zlo=zlo, mine=mine):
            at = pl.ds(pl.multiple_of(i * rows, 16), rows)
            q0 = own[at, 0:128].astype(F32) + received[at, 0:128].astype(F32)
            q1 = own[at, 128:256].astype(F32) + received[at, 128:256].astype(F32)
            o = own[at, 256:384].astype(F32) + received[at, 256:384].astype(F32)
            q1 = jnp.where(lane < QKV - 128, q1, pltpu.roll(o, QKV - 128, 1))
            low = jnp.zeros((part, 128), F32)
            high = jnp.zeros((part, 128), F32)
            for g in range(6):
                piece = pltpu.roll(o[g * part : (g + 1) * part], (32 * g - KEPT) % 128, 1)
                here = (few >= 32 * (g % 4)) & (few < 32 * (g % 4) + 32)
                if g < 4:
                    low = jnp.where(here, piece, low)
                else:
                    high = jnp.where(here, piece, high)
            dest = 2 * i + zlo
            out_ref[dest, 0:rows, 0:128] = q0.astype(BF16)
            out_ref[dest, 0:rows, 128:256] = q1.astype(BF16)
            out_ref[dest, rows : rows + part, 0:128] = low.astype(BF16)
            out_ref[dest, rows : rows + part, 128:256] = high.astype(BF16)
            right = act_ref[i, :, 128:256].astype(F32)
            right = jnp.where((side >= 16) & (side < 16 + HD), mine, right)
            out_ref[dest, rows + part :, 0:128] = act_ref[i, :, 0:128]
            out_ref[dest, rows + part :, 128:256] = right.astype(BF16)
            return carry

        lax.fori_loop(0, 8, block, 0)


def final_kernel(in_ref, gq, go, ga, side_ref):
    rows = gq.shape[0]
    part = rows // 6
    lane = lax.broadcasted_iota(jnp.int32, (part, 128), 1)

    def total(a, b, c):
        out = in_ref[0, a:b, c : c + 128].astype(F32)
        for i in range(1, in_ref.shape[0]):
            out = out + in_ref[i, a:b, c : c + 128].astype(F32)
        return out

    gq[:, 0:128] = total(0, rows, 0)
    right = total(0, rows, 128)
    gq[:, 128:QKV] = right[:, 0 : QKV - 128]
    rest = (total(rows, rows + part, 0), total(rows, rows + part, 128))
    first = pltpu.roll(right, 128 - (QKV - 128), 1)
    for g in range(6):
        tail = pltpu.roll(rest[g // 4], (KEPT - 32 * g) % 128, 1)
        both = jnp.where(lane < KEPT, first[g * part : (g + 1) * part], tail)
        go[g * part : (g + 1) * part, :] = both[:, 0:HD]
    for i in range(in_ref.shape[0]):
        side_ref[i * 16 : (i + 1) * 16, :] = in_ref[i, rows + part :, :]
    right = side_ref[:, 128:256]
    kind = lax.rem(lax.broadcasted_iota(jnp.int32, right.shape, 0), 8)
    for k in range(3):
        chosen = jnp.where(kind // 2 == k, right.astype(F32), 0.0).astype(BF16)
        grad = pltpu.roll(dot(side_ref[...], chosen, 0, 0)[:rows], 128 - 16, 1)
        ga[k] = grad[:, 0:HD]


def lookup_rows(indices, table_rows):
    one_hot = (
        indices[:, None] == jnp.arange(table_rows.shape[0], dtype=jnp.int32)[None, :]
    ).astype(table_rows.dtype)
    return jnp.dot(one_hot, table_rows, preferred_element_type=F32)


def unshuffled(pieces, zlo, core):
    outs = []
    for p in range(4):
        near = jnp.where(core == 0, pieces[p], pieces[p ^ 1])
        far = jnp.where(core == 0, pieces[p ^ 2], pieces[p ^ 3])
        outs.append(jnp.where(zlo == 0, near, far))
    return outs


def around(v):
    return tuple(lax.ppermute(v, "x", shifted(4, k)) for k in (1, 3, 2))


def all_heads(qkv_rows, out_rows, way):
    own = (qkv_rows, out_rows)
    near = tuple(lax.ppermute(v, "core", xored(2, 1)) for v in own)
    far = tuple(lax.ppermute(v, ("zhi", "zlo"), shifted(4, way)) for v in own)
    last = tuple(lax.ppermute(v, "core", xored(2, 1)) for v in far)
    width = qkv_rows.shape[1]
    return pl.pallas_call(
        assemble_kernel,
        out_shape=(
            jax.ShapeDtypeStruct((4 * QKV, width), BF16),
            jax.ShapeDtypeStruct((4 * HD, width), BF16),
        ),
        in_specs=[pl.BlockSpec(memory_space=pl.ANY)] * 8,
        out_specs=(VM, VM),
        scratch_shapes=[pltpu.SemaphoreType.DMA((8,))],
        compiler_params=params(8),
        cost_estimate=cost(2),
    )(*own, *near, *far, *last)


def local(
    noisy, labels, tsteps, guide_index, class_table, time_table, guide_table, guide_weights,
    teacher_qkv, teacher_out, teacher_ada, student_qkv, student_out, student_ada,
):
    samples, seq_len, part = noisy.shape
    width = part * 16
    block = width // 4
    x_at = lax.axis_index("x")
    zlo, core = lax.axis_index("zlo"), lax.axis_index("core")
    quad = zlo * 2 + core
    scale_norm = 1.0 / math.sqrt(samples * 8 * seq_len)
    pos = x_at.reshape(1).astype(jnp.int32)

    flipped = jnp.swapaxes(noisy, 1, 2)
    sent = [lax.dynamic_slice_in_dim(flipped, (quad ^ r) * 2, 2, 0) for r in range(4)]
    got = [sent[0]] + [lax.ppermute(sent[r], QUAD, xored(4, r)) for r in (3, 2, 1)][::-1]
    mine = jnp.concatenate(unshuffled(got, zlo, core), axis=1)
    tokens = (mine,) + around(mine)

    weights = (jnp.swapaxes(student_qkv, 0, 1), student_out, jnp.swapaxes(teacher_qkv, 0, 1), teacher_out)
    weights = lax.optimization_barrier((weights, sent))[0]
    wq_s, wo_s = all_heads(weights[0], weights[1], 3)
    wq_t, wo_t = all_heads(weights[2], weights[3], 1)

    null_class = class_table.shape[0] - 1
    time_embed = lookup_rows(tsteps, time_table)
    cond_embed = lookup_rows(labels, class_table) + time_embed
    null_embed = class_table[null_class].astype(F32)[None, :] + time_embed
    guide_hot = guide_index[:, None] == jnp.arange(guide_table.shape[0], dtype=jnp.int32)[None, :]
    student_embed = cond_embed + jnp.dot(
        guide_hot.astype(BF16), guide_table, preferred_element_type=F32
    )
    strength = jnp.sum(jnp.where(guide_hot, guide_weights[None, :], 0.0), axis=1)
    cond_act = jax.nn.silu(cond_embed).astype(BF16)
    null_act = jax.nn.silu(null_embed).astype(BF16)
    student_act = jax.nn.silu(student_embed).astype(BF16)
    mod_t = jnp.einsum(
        "bd,kde->bke", jnp.concatenate([cond_act, null_act], axis=0), teacher_ada, preferred_element_type=F32
    )
    mod_s = jnp.einsum("bd,kde->bke", student_act, student_ada, preferred_element_type=F32)
    mods = jnp.stack([mod_t[:samples], mod_t[samples:], mod_s], axis=1)
    mods = jnp.pad(mods.reshape(4, 18, part), ((0, 0), (0, 6), (0, 128 - part)))
    mods = jnp.broadcast_to(mods[None], (4, 4, 24, 128)).reshape(16, 24, 128)
    mods = lax.all_to_all(mods, TENSOR, split_axis=0, concat_axis=0, tiled=True)
    mods = jnp.swapaxes(mods[:, :18, :part], 1, 2).reshape(width, 18)
    strengths = lax.dynamic_slice_in_dim(strength, quad * 2, 2, 0)

    nd = lambda s, d=BF16: jax.ShapeDtypeStruct(s, d)
    saved = []
    for i in range(2):
        col = i * 9
        saved.append(
            pl.pallas_call(
                functools.partial(student_kernel, i, col + 6, scale_norm),
                out_shape=(
                    nd((width, seq_len)), nd((width, seq_len)), nd((4 * QKV, seq_len)),
                    nd((4, seq_len, seq_len)), nd((4 * HD, seq_len)), nd((width, seq_len)),
                    nd((width, seq_len), F32),
                ),
                in_specs=[SM] + [VM] * 7,
                out_specs=(VM,) * 7,
                scratch_shapes=[pltpu.VMEM((width, seq_len), BF16)],
                compiler_params=params(28),
                cost_estimate=cost(5),
            )(pos, *tokens, mods, wq_s, wo_s)
        )
    cots = []
    for i in range(2):
        col = i * 9
        coef = jnp.stack([-(1.0 + strengths[i]), strengths[i]]) * scale_norm
        o0, o1, o3, o2 = pl.pallas_call(
            functools.partial(teacher_kernel, (col, col + 3)),
            grid=(2,),
            out_shape=(nd((block, seq_len)),) * 4,
            in_specs=[SM, SM] + [VM] * 5,
            out_specs=(VM,) * 4,
            scratch_shapes=[
                pltpu.VMEM((width, seq_len), F32),
                pltpu.VMEM((width, seq_len), BF16),
                pltpu.VMEM((4 * QKV, seq_len), BF16),
                pltpu.VMEM((4 * HD, seq_len), BF16),
            ],
            compiler_params=params(24, dimension_semantics=("arbitrary",)),
            cost_estimate=cost(9),
        )(pos, coef, saved[i][0], mods, wq_t, wo_t, saved[i][6])
        terms = [o0] + [lax.ppermute(o, "x", shifted(4, k)) for o, k in ((o1, 1), (o3, 3), (o2, 2))]
        cot = functools.reduce(jnp.add, [t.astype(F32) for t in terms]).astype(BF16)
        cots.append((cot,) + around(cot))

    back = []
    for i in range(2):
        normed, _, qkv, prob, mixed, proj, _ = saved[i]
        back.append(
            pl.pallas_call(
                functools.partial(backward_kernel, i * 9 + 6),
                out_shape=(nd((width, seq_len)), nd((4 * QKV, seq_len)), nd((8, width), F32)),
                in_specs=[SM] + [VM] * 12,
                out_specs=(VM,) * 3,
                scratch_shapes=[
                    pltpu.VMEM((width, seq_len), BF16),
                    pltpu.VMEM((4 * HD, seq_len), BF16),
                    pltpu.VMEM((width, 128), F32),
                ],
                compiler_params=params(28),
                cost_estimate=cost(6),
            )(pos, *cots[i], mods, wq_s, wo_s, normed, qkv, prob, mixed, proj)
        )

    gm = jnp.stack([back[0][2][:3], back[1][2][:3]], axis=1).reshape(6, width)
    gm = jnp.pad(gm, ((0, 2), (0, 0)))
    gm = jnp.concatenate([gm, lax.ppermute(gm, "core", xored(2, 1))], axis=0)
    gm = (gm,) + around(gm)
    acts = []
    for q in (quad, quad ^ 1):
        two = lax.dynamic_slice_in_dim(student_act, q * 2, 2, 0)
        acts += [two, two, two, jnp.zeros_like(two)]
    act_blocks = jnp.swapaxes(jnp.concatenate(acts, axis=0).reshape(16, 8, width // 8), 0, 1)
    act_blocks = jnp.pad(act_blocks, ((0, 0), (0, 0), (0, 256 - width // 8)))

    operands = []
    for i in range(2):
        operands += [saved[i][1], back[i][1], back[i][0], saved[i][4]]
    far1, far3, near0, near2 = pl.pallas_call(
        grads_kernel,
        out_shape=(nd((width, LANES)),) * 4,
        in_specs=[VM] * 8,
        out_specs=(VM,) * 4,
        compiler_params=params(24),
        cost_estimate=cost(4),
        name="grads",
    )(*operands)
    received = [lax.ppermute(v, "core", xored(2, 1)) for v in (far1, far3)]
    rows = width // 8
    pieces = pl.pallas_call(
        fold_kernel,
        out_shape=nd((16, rows // 6 * 7 + 16, 256)),
        in_specs=[SM] + [VM] * 9,
        out_specs=VM,
        compiler_params=params(16),
        cost_estimate=cost(2),
        name="fold",
    )(jnp.stack([x_at, zlo, core]).astype(jnp.int32), near0, near2, *received, act_blocks, *gm)
    summed = lax.all_to_all(pieces, ("zhi", "y", "zlo"), split_axis=0, concat_axis=0, tiled=True)
    grad_qkv, grad_out, grad_ada = pl.pallas_call(
        final_kernel,
        out_shape=(nd((rows, QKV), F32), nd((rows, HD), F32), nd((3, rows, HD), F32)),
        in_specs=[VM],
        out_specs=(VM, VM, VM),
        scratch_shapes=[pltpu.VMEM((256, 256), BF16)],
        compiler_params=params(12),
        cost_estimate=cost(1),
        name="final",
    )(summed)
    grad_out = grad_out.T

    return (grad_qkv, grad_out, grad_ada)


def solution(mesh):
    fine = Mesh(mesh.devices.reshape(SIZES), AXES)
    return jax.shard_map(
        local,
        mesh=fine,
        in_specs=(
            P(DP, None, TENSOR), P(DP), P(DP), P(DP), P(), P(), P(), P(),
            P(None, TENSOR), P(TENSOR, None), P(None, None, TENSOR),
            P(None, TENSOR), P(TENSOR, None), P(None, None, TENSOR),
        ),
        out_specs=(P(DP, TENSOR), P(TENSOR, DP), P(None, DP, TENSOR)),
        check_vma=False,
    )
```
